64 devices in a mesh: dp: 4 (over x, y), vp: 16 (over z, core).
Axes of the slice: x: 2, y: 2, z: 8, core: 2. Of those that a mesh axis runs over, the one named last changes fastest.
The devices are a block of a 4x4x8 slice.
Arguments:
- hidden: bfloat16 [4096, 4096], P('dp'), parts along dimension 0
- w_head: bfloat16 [4096, 32768], P(None, 'vp')
- inv_temp: float32 [4096], P('dp'), parts along dimension 0
- target_ids: int32 [4096], P('dp'), parts along dimension 0
Outputs:
- output 1: float32 [4096, 32768], P(('dp', 'vp')), parts along dimension 0
- output 2: float32 [4096], P('dp'), parts along dimension 0
There are 4 independent parts. The reference program is written for one: setup_inputs(seed, part) draws one part's arguments, and reference() takes and returns one part's arrays. A program takes and returns all parts, laid end to end along the dimension named above; an argument that names none is the same for every part.
All inputs are finite; a program needn't handle non-finite values.
Results may differ from the reference program's by a relative error of at most 0.001.
Values are sent between devices in bfloat16 or wider.
A program may use at most 768 MiB of HBM per device.

```python
import math
import jax
import jax.numpy as jnp
from jax import lax

BATCH = 1024
HIDDEN = 4096
VOCAB = 32768
W_ROW_BLOCK = 256


def draw_head(key, direction, profile):
    num_blocks = HIDDEN // W_ROW_BLOCK
    dir_blocks = direction.reshape(num_blocks, W_ROW_BLOCK)

    def one_block(block_args):
        block_idx, dir_rows = block_args
        noise_rows = jax.random.normal(jax.random.fold_in(key, block_idx), (W_ROW_BLOCK, VOCAB), jnp.float32)
        head_rows = (noise_rows + dir_rows[:, None] * profile[None, :]) * (HIDDEN ** -0.5)
        return head_rows.astype(jnp.bfloat16)

    blocks = lax.map(one_block, (jnp.arange(num_blocks), dir_blocks))
    return blocks.reshape(HIDDEN, VOCAB)


def setup_inputs(seed: int = 0, part: int = 0) -> dict:
    base_key = jax.random.key(seed)
    shared_key = jax.random.fold_in(base_key, 1)
    part_key = jax.random.fold_in(jax.random.fold_in(base_key, 2), part)
    key_dir, key_head = jax.random.split(shared_key)
    key_hid, key_gain, key_temp, key_ids = jax.random.split(part_key, 4)
    direction = jax.random.normal(key_dir, (HIDDEN,), jnp.float32)
    vocab_pos = jnp.arange(VOCAB, dtype=jnp.float32) / VOCAB
    profile = 1.5 * jnp.exp(-8.0 * vocab_pos)
    w_head = draw_head(key_head, direction, profile)
    row_gain = 2.0 + 0.5 * jax.random.normal(key_gain, (BATCH, 1), jnp.float32)
    hidden = jax.random.normal(key_hid, (BATCH, HIDDEN), jnp.float32) + row_gain * direction[None, :] * (HIDDEN ** -0.5)
    row_pos = jnp.arange(BATCH)
    log_temp = jax.random.uniform(key_temp, (BATCH,), jnp.float32, minval=math.log(0.5), maxval=math.log(32.0))
    inv_temp = jnp.where(row_pos == 0, 32.0, jnp.exp(log_temp))
    target_ids = jax.random.randint(key_ids, (BATCH,), 0, VOCAB, dtype=jnp.int32)
    target_ids = jnp.where(row_pos == 1, VOCAB - 1, target_ids)
    return {"hidden": hidden.astype(jnp.bfloat16), "w_head": w_head, "inv_temp": inv_temp, "target_ids": target_ids}


def reference(hidden, w_head, inv_temp, target_ids):
    logits = jnp.dot(hidden, w_head, preferred_element_type=jnp.float32)
    scaled = logits * inv_temp[:, None]
    row_max = jnp.max(scaled, axis=1, keepdims=True)
    exp_vals = jnp.exp(scaled - row_max)
    probabilities = exp_vals / jnp.sum(exp_vals, axis=1, keepdims=True)
    cdf_table = jnp.cumsum(probabilities, axis=1)
    cdf_at_target = jnp.take_along_axis(cdf_table, target_ids[:, None], axis=1)[:, 0]
    return cdf_table, cdf_at_target
```

```python
import functools
import jax
import jax.numpy as jnp
from jax import lax
from jax.experimental import pallas as pl
from jax.experimental.pallas import tpu as pltpu
from jax.sharding import PartitionSpec as P

MESH = pl.DeviceIdType.MESH
F32 = jnp.float32
BF16 = jnp.bfloat16
CHUNKS = 4
LANES = 128


def exchange_kernel(
    size, it_ref, tgt_ref, hid_ref, w_ref,
    recv_ref, so_ref, out_t_ref,
    w_v, hid_v, tri_v, send_v, stat_send, stat_recv,
    w_sem, h_sem, data_send, data_recv, stat_ssem, stat_rsem, t_ssem, t_rsem,
):
    me = lax.axis_index("vp")
    chips = size // 2
    z, c = me // 2, me % 2
    rows = hid_ref.shape[0] // chips
    half = rows // 2
    depth = hid_ref.shape[1]
    local_vocab = w_ref.shape[1]
    width = local_vocab // CHUNKS
    block = tri_v.shape[0]

    def chip_at(i):
        dist = chips // 2 - (i + 1) // 2
        sign = 2 * (i % 2) - 1
        return (z + sign * dist + 2 * chips) % chips

    barrier = pltpu.get_barrier_semaphore()
    for k in range(1, size):
        pl.semaphore_signal(barrier, inc=1, device_id={"vp": (me + k) % size}, device_id_type=MESH)

    parts = 4
    piece = depth // parts

    def w_copy(j, p):
        return pltpu.make_async_copy(
            w_ref.at[pl.ds(p * piece, piece), pl.ds(pl.multiple_of(j * width, width), width)],
            w_v.at[j, pl.ds(p * piece, piece)],
            w_sem.at[j, p],
        )

    def h_copy(i):
        start = pl.multiple_of(chip_at(i) * rows, rows)
        return pltpu.make_async_copy(hid_ref.at[pl.ds(start, rows)], hid_v.at[i], h_sem.at[i])

    h_copy(0).start()
    for p in range(parts):
        w_copy(0, p).start()
    r_iota = lax.broadcasted_iota(jnp.int32, (block, block), 0)
    c_iota = lax.broadcasted_iota(jnp.int32, (block, block), 1)
    tri_v[...] = jnp.where(r_iota <= c_iota, 1.0, 0.0).astype(BF16)
    h_copy(0).wait()
    for p in range(parts):
        w_copy(0, p).wait()
    for j in range(1, CHUNKS):
        for p in range(parts):
            w_copy(j, p).start()
    for i in range(1, chips):
        h_copy(i).start()

    lane = lax.broadcasted_iota(jnp.int32, (rows, LANES), 1)

    def to_column(row):
        return jnp.transpose(jnp.broadcast_to(row, (LANES, LANES)))[:, :1]

    def row_params(i):
        chip = chip_at(i)
        temp = to_column(it_ref[pl.ds(chip, 1)])
        target = to_column((tgt_ref[pl.ds(chip, 1)] - me * local_vocab).astype(F32))
        return temp, target

    def chunk(i, j, temp, target, state):
        top, carry, pick, stats = state
        logits = jnp.dot(hid_v[i], w_v[j], preferred_element_type=F32) * temp
        new_top = jnp.maximum(top, jnp.max(logits, axis=1, keepdims=True))
        drop = jnp.exp(top - new_top)
        carry = carry * drop
        pick = pick * drop
        e = jnp.exp(logits - new_top)
        first = e.astype(BF16)
        rest = e - first.astype(F32)
        second = rest.astype(BF16)
        third = (rest - second.astype(F32)).astype(BF16)
        col = lax.broadcasted_iota(jnp.int32, (rows, block), 1).astype(F32)
        base = (j * width).astype(F32) if not isinstance(j, int) else float(j * width)
        for t in range(width // block):
            cut = slice(t * block, (t + 1) * block)
            terms = jnp.concatenate([first[:, cut], second[:, cut], third[:, cut]], axis=0)
            sums = jnp.dot(terms, tri_v[...], preferred_element_type=F32)
            run = (sums[:rows] + (sums[rows : 2 * rows] + sums[2 * rows :])) + carry
            send_v[i, j, :, pl.ds(t * block, block)] = run
            hit = (col + (base + float(t * block))) == target
            pick = pick + jnp.sum(jnp.where(hit, run, 0.0), axis=1, keepdims=True)
            carry = run[:, block - 1 :]
        stats = jnp.where(lane == j, new_top, stats)
        return new_top, carry, pick, stats

    def send_data(i, j):
        for core in range(2):
            pltpu.make_async_remote_copy(
                src_ref=send_v.at[i, j, pl.ds(core * half, half)],
                dst_ref=recv_ref.at[me * CHUNKS + j],
                send_sem=data_send.at[i],
                recv_sem=data_recv.at[me],
                device_id={"vp": chip_at(i) * 2 + core},
                device_id_type=MESH,
            ).start()

    def start_state():
        column = jnp.zeros((rows, 1), F32)
        return column - jnp.inf, column, column, jnp.zeros((rows, LANES), F32)

    def finish(i, state):
        _, carry, pick, stats = state
        stats = jnp.where(lane == CHUNKS, carry, stats)
        stats = jnp.where(lane == CHUNKS + 1, pick, stats)
        stat_send[i] = jnp.transpose(stats)[:8]

    temp0, target0 = row_params(0)
    state0 = chunk(0, 0, temp0, target0, start_state())
    pl.semaphore_wait(barrier, size - 1)
    send_data(0, 0)

    def first_step(j, state):
        for p in range(parts):
            w_copy(j, p).wait()
        state = chunk(0, j, temp0, target0, state)
        send_data(0, j)
        return state

    finish(0, lax.fori_loop(1, CHUNKS, first_step, state0))

    early = 3

    def step(i, carry_):
        h_copy(i).wait()
        temp, target = row_params(i)

        def inner(j, state):
            state = chunk(i, j, temp, target, state)

            @pl.when(i < early)
            def _():
                send_data(i, j)

            return state

        finish(i, lax.fori_loop(0, CHUNKS, inner, start_state()))
        return carry_

    lax.fori_loop(1, chips, step, 0)
    last = chips - 1

    def stat_copy(i, core):
        return pltpu.make_async_remote_copy(
            src_ref=stat_send.at[i],
            dst_ref=stat_recv.at[me],
            send_sem=stat_ssem.at[i * 2 + core],
            recv_sem=stat_rsem.at[me],
            device_id={"vp": chip_at(i) * 2 + core},
            device_id_type=MESH,
        )

    def partner_stat():
        return pltpu.make_async_remote_copy(
            src_ref=stat_send.at[last],
            dst_ref=stat_recv.at[me],
            send_sem=stat_ssem.at[last * 2],
            recv_sem=stat_rsem.at[me],
            device_id={"vp": z * 2 + (1 - c)},
            device_id_type=MESH,
        )

    for i in range(last):
        for core in range(2):
            stat_copy(i, core).start()
    partner_stat().start()
    stat_recv[me] = stat_send[last]

    def send_step(i, carry_):
        for j in range(CHUNKS):
            send_data(i, j)
        return carry_

    lax.fori_loop(early, early + 2, send_step, 0)

    def partner_data(j):
        return pltpu.make_async_remote_copy(
            src_ref=send_v.at[last, j, pl.ds(pl.multiple_of((1 - c) * half, half), half)],
            dst_ref=recv_ref.at[me * CHUNKS + j],
            send_sem=data_send.at[last],
            recv_sem=data_recv.at[me],
            device_id={"vp": z * 2 + (1 - c)},
            device_id_type=MESH,
        )

    for j in range(CHUNKS):
        partner_data(j).start()
    for j in range(CHUNKS):
        recv_ref[me * CHUNKS + j] = send_v[last, j, pl.ds(pl.multiple_of(c * half, half), half)]

    def wait_stat(k, carry_):
        src = (me + k) % size
        pltpu.make_async_remote_copy(
            src_ref=stat_send.at[0], dst_ref=stat_recv.at[src],
            send_sem=stat_ssem.at[0], recv_sem=stat_rsem.at[src],
            device_id={"vp": src}, device_id_type=MESH,
        ).wait_recv()
        return carry_

    lax.fori_loop(1, size, wait_stat, 0)
    tops = [stat_recv[s, CHUNKS - 1 : CHUNKS] for s in range(size)]
    global_top = functools.reduce(jnp.maximum, tops)
    weights = [jnp.exp(t - global_top) for t in tops]
    masses = [stat_recv[s, CHUNKS : CHUNKS + 1] * weights[s] for s in range(size)]
    inverse = 1.0 / functools.reduce(lambda a, b: a + b, masses)
    offsets = [jnp.zeros((1, rows), F32)]
    for s in range(size - 1):
        offsets.append(offsets[-1] + masses[s])
    ids = tgt_ref[pl.ds(z, 1)]
    value = jnp.zeros((1, rows), F32)
    for s in range(size):
        inside = (ids >= s * local_vocab) & (ids < (s + 1) * local_vocab)
        here = stat_recv[s, CHUNKS + 1 : CHUNKS + 2] * weights[s] + offsets[s]
        value = value + jnp.where(inside, here, 0.0)
    out_t_ref[pl.ds(z, 1)] = value * inverse

    def t_copy(k):
        return pltpu.make_async_remote_copy(
            src_ref=out_t_ref.at[pl.ds(z, 1)],
            dst_ref=out_t_ref.at[pl.ds(z, 1)],
            send_sem=t_ssem.at[k],
            recv_sem=t_rsem.at[z],
            device_id={"vp": ((z + k) % chips) * 2 + c},
            device_id_type=MESH,
        )

    for k in range(1, chips):
        t_copy(k).start()

    lax.fori_loop(early + 2, last, send_step, 0)

    scales = [jnp.exp(stat_recv[s, :CHUNKS] - global_top) * inverse for s in range(size)]
    table = jnp.concatenate(scales + [o * inverse for o in offsets], axis=0)
    pad = LANES - table.shape[0]
    if pad:
        table = jnp.concatenate([table, jnp.zeros((pad, rows), F32)], axis=0)
    turned = jnp.transpose(table)
    so_ref[...] = jnp.where(c == 0, turned[:half], turned[half:])

    def wait_sends(i, carry_):
        pltpu.make_async_remote_copy(
            src_ref=send_v.at[i], dst_ref=send_v.at[i], send_sem=data_send.at[i], recv_sem=data_recv.at[0],
            device_id={"vp": chip_at(i) * 2}, device_id_type=MESH,
        ).wait_send()
        for core in range(2):
            stat_copy(i, core).wait_send()
        return carry_

    lax.fori_loop(0, last, wait_sends, 0)
    partner_stat().wait_send()
    for k in range(1, chips):
        t_copy(k).wait_send()
    mine = pl.ds(pl.multiple_of((1 - c) * half, half), half)
    pltpu.make_async_remote_copy(
        src_ref=send_v.at[last, :, mine], dst_ref=send_v.at[last, :, mine],
        send_sem=data_send.at[last], recv_sem=data_recv.at[0],
        device_id={"vp": z * 2 + (1 - c)}, device_id_type=MESH,
    ).wait_send()

    def wait_t(k, carry_):
        src = (z + k) % chips
        pltpu.make_async_remote_copy(
            src_ref=out_t_ref.at[pl.ds(src, 1)], dst_ref=out_t_ref.at[pl.ds(src, 1)],
            send_sem=t_ssem.at[0], recv_sem=t_rsem.at[src],
            device_id={"vp": src * 2 + c}, device_id_type=MESH,
        ).wait_recv()
        return carry_

    lax.fori_loop(1, chips, wait_t, 0)

    def wait_data(k, carry_):
        src = (me + k) % size
        there = recv_ref.at[pl.ds(src * CHUNKS, CHUNKS)]
        pltpu.make_async_remote_copy(
            src_ref=there, dst_ref=there, send_sem=data_send.at[0], recv_sem=data_recv.at[src],
            device_id={"vp": src}, device_id_type=MESH,
        ).wait_recv()
        return carry_

    lax.fori_loop(1, size, wait_data, 0)


def table_kernel(size, recv_ref, so_ref, t_ref, table_ref, out_t_ref, stage, sems, t_sem):
    width = recv_ref.shape[2]
    t_out = pltpu.make_async_copy(t_ref, out_t_ref, t_sem)
    t_out.start()
    copies = []
    for s in range(size):
        offset = so_ref[:, size * CHUNKS + s : size * CHUNKS + s + 1]
        for j in range(CHUNKS):
            k = s * CHUNKS + j
            stage[s, :, j * width : (j + 1) * width] = recv_ref[k] * so_ref[:, k : k + 1] + offset
        shard = CHUNKS * width
        copy = pltpu.make_async_copy(stage.at[s], table_ref.at[:, pl.ds(s * shard, shard)], sems.at[s])
        copy.start()
        copies.append(copy)
    t_out.wait()
    for copy in copies:
        copy.wait()


def solution(mesh):
    size = mesh.shape["vp"]
    chips = size // 2

    def local_step(hidden, w_local, inv_temp, target_ids):
        batch, depth = hidden.shape
        local_vocab = w_local.shape[1]
        width = local_vocab // CHUNKS
        rows = batch // chips
        half = rows // 2
        block = min(256, width)
        vmem = pl.BlockSpec(memory_space=pltpu.VMEM)
        hbm = pl.BlockSpec(memory_space=pl.ANY)
        recv, so, t_all = pl.pallas_call(
            functools.partial(exchange_kernel, size),
            out_shape=(
                pltpu.VMEM((size * CHUNKS, half, width), F32),
                pltpu.VMEM((half, LANES), F32),
                pltpu.VMEM((chips, rows), F32),
            ),
            in_specs=[vmem, vmem, hbm, hbm],
            out_specs=(vmem, vmem, vmem),
            scratch_shapes=[
                pltpu.VMEM((CHUNKS, depth, width), BF16),
                pltpu.VMEM((chips, rows, depth), BF16),
                pltpu.VMEM((block, block), BF16),
                pltpu.VMEM((chips, CHUNKS, rows, width), F32),
                pltpu.VMEM((chips, 8, rows), F32),
                pltpu.VMEM((size, 8, rows), F32),
                pltpu.SemaphoreType.DMA((CHUNKS, 4)),
                pltpu.SemaphoreType.DMA((chips,)),
                pltpu.SemaphoreType.DMA((chips,)),
                pltpu.SemaphoreType.DMA((size,)),
                pltpu.SemaphoreType.DMA((size,)),
                pltpu.SemaphoreType.DMA((size,)),
                pltpu.SemaphoreType.DMA((chips,)),
                pltpu.SemaphoreType.DMA((chips,)),
            ],
            compiler_params=pltpu.CompilerParams(
                collective_id=0, has_side_effects=True, vmem_limit_bytes=46 * 1024 * 1024
            ),
            name="exchange",
        )(inv_temp.reshape(chips, rows), target_ids.reshape(chips, rows), hidden, w_local)
        recv, so, t_all = [pltpu.with_memory_space_constraint(x, pltpu.VMEM) for x in (recv, so, t_all)]
        table, cdf_at_target = pl.pallas_call(
            functools.partial(table_kernel, size),
            out_shape=(
                jax.ShapeDtypeStruct((half, size * local_vocab), F32),
                jax.ShapeDtypeStruct((chips, rows), F32),
            ),
            in_specs=[vmem, vmem, vmem],
            out_specs=(hbm, hbm),
            scratch_shapes=[
                pltpu.VMEM((size, half, local_vocab), F32),
                pltpu.SemaphoreType.DMA((size,)),
                pltpu.SemaphoreType.DMA,
            ],
            compiler_params=pltpu.CompilerParams(vmem_limit_bytes=24 * 1024 * 1024),
            name="table",
        )(recv, so, t_all)
        return table, cdf_at_target.reshape(batch)

    return jax.shard_map(
        local_step,
        mesh=mesh,
        in_specs=(P("dp", None), P(None, "vp"), P("dp"), P("dp")),
        out_specs=(P(("dp", "vp"), None), P("dp")),
        check_vma=False,
    )
```

```python
import functools
import jax
import jax.numpy as jnp
from jax import lax
from jax.experimental import pallas as pl
from jax.experimental.pallas import tpu as pltpu
from jax.sharding import PartitionSpec as P

MESH = pl.DeviceIdType.MESH
F32 = jnp.float32
BF16 = jnp.bfloat16
LANES = 128
EIGHTHS = (1, 3, 4)
CHUNKS = len(EIGHTHS)
STATS = CHUNKS + 2


def chunk_bounds(local_vocab):
    bounds, start = [], 0
    for part in EIGHTHS:
        bounds.append((start, part * local_vocab // 8))
        start += part * local_vocab // 8
    return bounds


def exchange_kernel(
    size, it_hbm, tgt_hbm, hid_ref, w_ref,
    recv_ref, so_ref, out_t_ref,
    it_ref, tgt_ref, w_v, hid_v, tri_v, send_v, stat_mine, stat_recv, t_mine, t_recv,
    row_sem, w_sem, h_sem, h0_sem, data_send, data_recv, stat_ssem, stat_rsem, pair_ssem, pair_rsem, t_ssem, t_rsem,
):
    me = lax.axis_index("vp")
    chips = size // 2
    z, c = me // 2, me % 2
    rows = hid_ref.shape[0] // chips
    half = rows // 2
    depth = hid_ref.shape[1]
    local_vocab = w_ref.shape[1]
    bounds = chunk_bounds(local_vocab)
    block = tri_v.shape[0]

    pairs = chips // 2

    def chip_at(p, side):
        steps = pairs - 1 - p
        return (z + steps) % chips if side == 0 else (z - steps + pairs * (p // (pairs - 1)) + chips) % chips

    barrier = pltpu.get_barrier_semaphore()
    parts = w_sem.shape[1]
    piece = depth // parts

    def w_copy(j, p):
        start, width = bounds[j]
        here = (pl.ds(p * piece, piece), pl.ds(start, width))
        return pltpu.make_async_copy(w_ref.at[here], w_v.at[here], w_sem.at[j, p])

    def h_copy(p, side):
        start = pl.multiple_of(chip_at(p, side) * rows, rows)
        return pltpu.make_async_copy(
            hid_ref.at[pl.ds(start, rows)], hid_v.at[p, pl.ds(side * rows, rows)], h_sem.at[p, side]
        )

    def h_first(q, side):
        start = pl.multiple_of(chip_at(0, side) * rows, rows)
        here = pl.ds(q * piece, piece)
        return pltpu.make_async_copy(
            hid_ref.at[pl.ds(start, rows), here], hid_v.at[0, pl.ds(side * rows, rows), here], h0_sem.at[q, side]
        )

    row_copies = [
        pltpu.make_async_copy(it_hbm, it_ref, row_sem.at[0]),
        pltpu.make_async_copy(tgt_hbm, tgt_ref, row_sem.at[1]),
    ]
    for q in range(parts):
        for side in range(2):
            h_first(q, side).start()
        w_copy(0, q).start()
    for copy in row_copies:
        copy.start()
    for k in range(1, size):
        pl.semaphore_signal(barrier, inc=1, device_id={"vp": (me + k) % size}, device_id_type=MESH)
    r_iota = lax.broadcasted_iota(jnp.int32, (block, block), 0)
    c_iota = lax.broadcasted_iota(jnp.int32, (block, block), 1)
    tri_v[...] = jnp.where(r_iota <= c_iota, 1.0, 0.0).astype(BF16)

    lane = lax.broadcasted_iota(jnp.int32, (2 * rows, LANES), 1)

    def to_column(row):
        return jnp.transpose(jnp.broadcast_to(row, (LANES, LANES)))[:, :1]

    def row_params(p):
        chip = [chip_at(p, side) for side in range(2)]
        temp = [to_column(it_ref[pl.ds(k, 1)]) for k in chip]
        target = [to_column((tgt_ref[pl.ds(k, 1)] - me * local_vocab).astype(F32)) for k in chip]
        return jnp.concatenate(temp, axis=0), jnp.concatenate(target, axis=0)

    def product(p, j):
        start, width = bounds[j]
        return jnp.dot(hid_v[p], w_v[:, start : start + width], preferred_element_type=F32)

    def first_product():
        width = bounds[0][1]
        total = jnp.zeros((2 * rows, width), F32)
        for q in range(parts):
            for side in range(2):
                h_first(q, side).wait()
            w_copy(0, q).wait()
            w_copy(1, q).start()
            here = slice(q * piece, (q + 1) * piece)
            total = total + jnp.dot(hid_v[0, :, here], w_v[here, :width], preferred_element_type=F32)
        return total

    def chunk(p, j, logits, temp, target, state):
        top, carry, pick, stats = state
        first_col, width = bounds[j]
        logits = logits * temp
        new_top = jnp.maximum(top, jnp.max(logits, axis=1, keepdims=True))
        drop = jnp.exp(top - new_top)
        carry = carry * drop
        pick = pick * drop
        e = jnp.exp(logits - new_top)
        first = e.astype(BF16)
        rest = e - first.astype(F32)
        second = rest.astype(BF16)
        third = (rest - second.astype(F32)).astype(BF16)
        col = lax.broadcasted_iota(jnp.int32, (2 * rows, block), 1).astype(F32)
        for t in range(width // block):
            cut = slice(t * block, (t + 1) * block)
            terms = jnp.concatenate([first[:, cut], second[:, cut], third[:, cut]], axis=0)
            sums = jnp.dot(terms, tri_v[...], preferred_element_type=F32)
            run = (sums[: 2 * rows] + (sums[2 * rows : 4 * rows] + sums[4 * rows :])) + carry
            base = first_col + t * block
            send_v[p, :, base : base + block] = run
            hit = (col + float(base)) == target
            pick = pick + jnp.sum(jnp.where(hit, run, 0.0), axis=1, keepdims=True)
            carry = run[:, block - 1 :]
        stats = jnp.where(lane == j, new_top, stats)
        return new_top, carry, pick, stats

    def send(p, side, columns):
        for core in range(2):
            pltpu.make_async_remote_copy(
                src_ref=send_v.at[p, pl.ds(side * rows + core * half, half), columns],
                dst_ref=recv_ref.at[me, :, columns],
                send_sem=data_send.at[p, side],
                recv_sem=data_recv.at[me],
                device_id={"vp": chip_at(p, side) * 2 + core},
                device_id_type=MESH,
            ).start()

    whole = pl.ds(0, local_vocab)

    def start_state():
        column = jnp.zeros((2 * rows, 1), F32)
        return column - jnp.inf, column, column, jnp.zeros((2 * rows, LANES), F32)

    def finish(p, state):
        _, carry, pick, stats = state
        stats = jnp.where(lane == CHUNKS, carry, stats)
        stats = jnp.where(lane == CHUNKS + 1, pick, stats)
        for side in range(2):
            stat_mine[c, p, side] = jnp.transpose(stats[side * rows : (side + 1) * rows])[:STATS]

    for copy in row_copies:
        copy.wait()
    temp0, target0 = row_params(0)
    state = chunk(0, 0, first_product(), temp0, target0, start_state())
    pl.semaphore_wait(barrier, size - 1)
    for side in range(2):
        send(0, side, pl.ds(*bounds[0]))
    for j in range(2, CHUNKS):
        for q in range(parts):
            w_copy(j, q).start()
    for p in range(1, pairs):
        for side in range(2):
            h_copy(p, side).start()
    for j in range(1, CHUNKS):
        for q in range(parts):
            w_copy(j, q).wait()
        state = chunk(0, j, product(0, j), temp0, target0, state)
        for side in range(2):
            send(0, side, pl.ds(*bounds[j]))
    finish(0, state)

    def step(p, carry_):
        for side in range(2):
            h_copy(p, side).wait()
        temp, target = row_params(p)
        state = start_state()
        for j in range(CHUNKS):
            state = chunk(p, j, product(p, j), temp, target, state)
        finish(p, state)
        return carry_

    lax.fori_loop(1, pairs, step, 0)
    two, one, ends = range(1, pairs)
    others = [(p, side) for p in range(pairs) for side in range(2) if (p, side) != (ends, 0)]

    partner = z * 2 + (1 - c)

    def swap(k, mine, theirs):
        there = pltpu.make_async_remote_copy(
            src_ref=mine, dst_ref=mine, send_sem=pair_ssem.at[k], recv_sem=pair_rsem.at[k],
            device_id={"vp": partner}, device_id_type=MESH,
        )
        here = pltpu.make_async_remote_copy(
            src_ref=theirs, dst_ref=theirs, send_sem=pair_ssem.at[k], recv_sem=pair_rsem.at[k],
            device_id={"vp": partner}, device_id_type=MESH,
        )
        there.start()
        there.wait_send()
        here.wait_recv()

    swap(0, stat_mine.at[c], stat_mine.at[1 - c])

    def chip_on_side(p):
        steps = pairs - 1 - p
        return (z + (1 - 2 * c) * steps + c * pairs * (p // (pairs - 1)) + chips) % chips

    def stat_copy(p):
        return pltpu.make_async_remote_copy(
            src_ref=stat_mine.at[:, p, c],
            dst_ref=stat_recv.at[c, :, p],
            send_sem=stat_ssem.at[p],
            recv_sem=stat_rsem.at[p],
            device_id={"vp": chip_on_side(p) * 2 + c},
            device_id_type=MESH,
        )

    def t_copy(p):
        return pltpu.make_async_remote_copy(
            src_ref=t_mine,
            dst_ref=t_recv.at[c, pl.ds(p, 1)],
            send_sem=t_ssem.at[p],
            recv_sem=t_rsem.at[p],
            device_id={"vp": chip_on_side(p) * 2 + c},
            device_id_type=MESH,
        )

    def slot(chip):
        steps = (z - chip + chips) % chips
        side = steps // pairs
        return side, (1 - side) * (pairs - 1 - steps % pairs) + side * ((steps + pairs - 1) % pairs)

    for p in range(ends):
        stat_copy(p).start()

    @pl.when(c == 0)
    def _():
        stat_recv[0, :, ends] = stat_mine[:, ends, 0]

    @pl.when(c == 1)
    def _():
        stat_copy(ends).start()

    for side in range(2):
        send(one, side, whole)
    send(ends, 1, whole)

    theirs = pl.ds(pl.multiple_of((1 - c) * half, half), half)
    mine = pl.ds(pl.multiple_of(c * half, half), half)
    partner_data = pltpu.make_async_remote_copy(
        src_ref=send_v.at[ends, theirs],
        dst_ref=recv_ref.at[me],
        send_sem=data_send.at[ends, 0],
        recv_sem=data_recv.at[me],
        device_id={"vp": partner},
        device_id_type=MESH,
    )
    partner_data.start()
    recv_ref[me] = send_v[ends, mine]

    for p in range(ends):
        stat_copy(p).wait_recv()

    @pl.when(c == 1)
    def _():
        stat_copy(ends).wait_recv()

    swap(1, stat_recv.at[c], stat_recv.at[1 - c])
    shards = []
    for chip in range(chips):
        side, pair = slot(chip)
        shards += [stat_recv[side, core, pair] for core in range(2)]
    tops = [x[CHUNKS - 1 : CHUNKS] for x in shards]
    global_top = functools.reduce(jnp.maximum, tops)
    weights = [jnp.exp(t - global_top) for t in tops]
    masses = [x[CHUNKS : CHUNKS + 1] * w for x, w in zip(shards, weights)]
    inverse = 1.0 / functools.reduce(lambda a, b: a + b, masses)
    offsets = [jnp.zeros((1, rows), F32)]
    for s in range(size - 1):
        offsets.append(offsets[-1] + masses[s])
    ids = tgt_ref[pl.ds(z, 1)]
    value = jnp.zeros((1, rows), F32)
    for s in range(size):
        inside = (ids >= s * local_vocab) & (ids < (s + 1) * local_vocab)
        here = shards[s][CHUNKS + 1 : CHUNKS + 2] * weights[s] + offsets[s]
        value = value + jnp.where(inside, here, 0.0)
    t_mine[...] = value * inverse
    for p in range(ends):
        t_copy(p).start()

    @pl.when(c == 0)
    def _():
        t_recv[0, ends : ends + 1] = t_mine[...]

    @pl.when(c == 1)
    def _():
        t_copy(ends).start()

    for side in range(2):
        send(two, side, whole)

    scales = [jnp.exp(x[:CHUNKS] - global_top) * inverse for x in shards]
    table = jnp.concatenate(scales + [o * inverse for o in offsets], axis=0)
    pad = LANES - table.shape[0]
    if pad:
        table = jnp.concatenate([table, jnp.zeros((pad, rows), F32)], axis=0)
    turned = jnp.transpose(table)
    so_ref[...] = jnp.where(c == 0, turned[:half], turned[half:])

    for p in range(ends):
        t_copy(p).wait_recv()

    @pl.when(c == 1)
    def _():
        t_copy(ends).wait_recv()

    swap(2, t_recv.at[c], t_recv.at[1 - c])
    for chip in range(chips):
        side, pair = slot(chip)
        out_t_ref[chip : chip + 1] = t_recv[side, pl.ds(pair, 1)]
    for p in range(ends):
        stat_copy(p).wait_send()
        t_copy(p).wait_send()

    @pl.when(c == 1)
    def _():
        stat_copy(ends).wait_send()
        t_copy(ends).wait_send()

    for p, side in others:
        gone = send_v.at[p, pl.ds(side * rows, rows)]
        pltpu.make_async_remote_copy(
            src_ref=gone, dst_ref=gone, send_sem=data_send.at[p, side], recv_sem=data_recv.at[0],
            device_id={"vp": chip_at(p, side) * 2}, device_id_type=MESH,
        ).wait_send()
    partner_data.wait_send()

    def wait_data(k, carry_):
        src = (me + k) % size
        there = recv_ref.at[src]
        pltpu.make_async_remote_copy(
            src_ref=there, dst_ref=there, send_sem=data_send.at[0, 0], recv_sem=data_recv.at[src],
            device_id={"vp": src}, device_id_type=MESH,
        ).wait_recv()
        return carry_

    lax.fori_loop(1, size, wait_data, 0)


def table_kernel(size, recv_ref, so_ref, t_ref, table_ref, out_t_ref, stage, sems, t_sem):
    shard = recv_ref.shape[2]
    t_out = pltpu.make_async_copy(t_ref, out_t_ref, t_sem)
    t_out.start()
    copies = []
    for s in range(size):
        offset = so_ref[:, size * CHUNKS + s : size * CHUNKS + s + 1]
        for j, (start, width) in enumerate(chunk_bounds(shard)):
            k = s * CHUNKS + j
            cut = slice(start, start + width)
            stage[s, :, cut] = recv_ref[s, :, cut] * so_ref[:, k : k + 1] + offset
        copy = pltpu.make_async_copy(stage.at[s], table_ref.at[:, pl.ds(s * shard, shard)], sems.at[s])
        copy.start()
        copies.append(copy)
    t_out.wait()
    for copy in copies:
        copy.wait()


def solution(mesh):
    size = mesh.shape["vp"]
    chips = size // 2
    assert chips == 8

    def local_step(hidden, w_local, inv_temp, target_ids):
        batch, depth = hidden.shape
        local_vocab = w_local.shape[1]
        rows = batch // chips
        half = rows // 2
        block = min(256, local_vocab // 8)
        vmem = pl.BlockSpec(memory_space=pltpu.VMEM)
        hbm = pl.BlockSpec(memory_space=pl.ANY)
        recv, so, t_all = pl.pallas_call(
            functools.partial(exchange_kernel, size),
            out_shape=(
                pltpu.VMEM((size, half, local_vocab), F32),
                pltpu.VMEM((half, LANES), F32),
                pltpu.VMEM((chips, rows), F32),
            ),
            in_specs=[hbm, hbm, hbm, hbm],
            out_specs=(vmem, vmem, vmem),
            scratch_shapes=[
                pltpu.VMEM((chips, rows), F32),
                pltpu.VMEM((chips, rows), jnp.int32),
                pltpu.VMEM((depth, local_vocab), BF16),
                pltpu.VMEM((chips // 2, 2 * rows, depth), BF16),
                pltpu.VMEM((block, block), BF16),
                pltpu.VMEM((chips // 2, 2 * rows, local_vocab), F32),
                pltpu.VMEM((2, chips // 2, 2, STATS, rows), F32),
                pltpu.VMEM((2, 2, chips // 2, STATS, rows), F32),
                pltpu.VMEM((1, rows), F32),
                pltpu.VMEM((2, chips // 2, rows), F32),
                pltpu.SemaphoreType.DMA((2,)),
                pltpu.SemaphoreType.DMA((CHUNKS, 4)),
                pltpu.SemaphoreType.DMA((chips // 2, 2)),
                pltpu.SemaphoreType.DMA((4, 2)),
                pltpu.SemaphoreType.DMA((chips // 2, 2)),
                pltpu.SemaphoreType.DMA((size,)),
                pltpu.SemaphoreType.DMA((chips // 2,)),
                pltpu.SemaphoreType.DMA((chips // 2,)),
                pltpu.SemaphoreType.DMA((3,)),
                pltpu.SemaphoreType.DMA((3,)),
                pltpu.SemaphoreType.DMA((chips // 2,)),
                pltpu.SemaphoreType.DMA((chips // 2,)),
            ],
            compiler_params=pltpu.CompilerParams(
                collective_id=0, has_side_effects=True, vmem_limit_bytes=46 * 1024 * 1024
            ),
            name="exchange",
        )(inv_temp.reshape(chips, rows), target_ids.reshape(chips, rows), hidden, w_local)
        recv, so, t_all = [pltpu.with_memory_space_constraint(x, pltpu.VMEM) for x in (recv, so, t_all)]
        table, cdf_at_target = pl.pallas_call(
            functools.partial(table_kernel, size),
            out_shape=(
                jax.ShapeDtypeStruct((half, size * local_vocab), F32),
                jax.ShapeDtypeStruct((chips, rows), F32),
            ),
            in_specs=[vmem, vmem, vmem],
            out_specs=(hbm, hbm),
            scratch_shapes=[
                pltpu.VMEM((size, half, local_vocab), F32),
                pltpu.SemaphoreType.DMA((size,)),
                pltpu.SemaphoreType.DMA,
            ],
            compiler_params=pltpu.CompilerParams(vmem_limit_bytes=24 * 1024 * 1024),
            name="table",
        )(recv, so, t_all)
        return table, cdf_at_target.reshape(batch)

    return jax.shard_map(
        local_step,
        mesh=mesh,
        in_specs=(P("dp", None), P(None, "vp"), P("dp"), P("dp")),
        out_specs=(P(("dp", "vp"), None), P("dp")),
        check_vma=False,
    )
```

```python
import functools
import jax
import jax.numpy as jnp
from jax import lax
from jax.experimental import pallas as pl
from jax.experimental.pallas import tpu as pltpu
from jax.sharding import PartitionSpec as P

MESH = pl.DeviceIdType.MESH
F32 = jnp.float32
BF16 = jnp.bfloat16
LANES = 128
EIGHTHS = (1, 3, 4)
CHUNKS = len(EIGHTHS)
STATS = CHUNKS + 2


def chunk_bounds(local_vocab):
    bounds, start = [], 0
    for part in EIGHTHS:
        bounds.append((start, part * local_vocab // 8))
        start += part * local_vocab // 8
    return bounds


def exchange_kernel(
    size, it_hbm, tgt_hbm, hid_ref, w_ref,
    recv_ref, so_ref, out_t_ref,
    it_ref, tgt_ref, w_v, hid_v, tri_v, state_v, send_v, stat_mine, stat_recv, t_mine, t_recv,
    row_sem, w_sem, h_sem, h0_sem, data_send, data_recv, stat_ssem, stat_rsem, pair_ssem, pair_rsem, t_ssem, t_rsem,
):
    me = lax.axis_index("vp")
    chips = size // 2
    z, c = me // 2, me % 2
    rows = hid_ref.shape[0] // chips
    half = rows // 2
    depth = hid_ref.shape[1]
    local_vocab = w_ref.shape[1]
    bounds = chunk_bounds(local_vocab)
    block = tri_v.shape[0]

    pairs = chips // 2

    def chip_at(p, side):
        steps = pairs - 1 - p
        return (z + steps) % chips if side == 0 else (z - steps + pairs * (p // (pairs - 1)) + chips) % chips

    barrier = pltpu.get_barrier_semaphore()
    parts = w_sem.shape[1]
    piece = depth // parts

    def w_copy(j, p):
        start, width = bounds[j]
        here = (pl.ds(pl.multiple_of(p * piece, piece), piece), pl.ds(start, width))
        return pltpu.make_async_copy(w_ref.at[here], w_v.at[here], w_sem.at[j, p])

    def h_copy(p, side):
        start = pl.multiple_of(chip_at(p, side) * rows, rows)
        return pltpu.make_async_copy(
            hid_ref.at[pl.ds(start, rows)], hid_v.at[p, pl.ds(side * rows, rows)], h_sem.at[p, side]
        )

    def h_first(q, side):
        chip = chip_at(0, 0) * (1 - side) + chip_at(0, 1) * side
        start = pl.multiple_of(chip * rows, rows)
        here = pl.ds(pl.multiple_of(q * piece, piece), piece)
        there = pl.ds(pl.multiple_of(side * rows, rows), rows)
        return pltpu.make_async_copy(
            hid_ref.at[pl.ds(start, rows), here], hid_v.at[0, there, here], h0_sem.at[q, side]
        )

    row_copies = [
        pltpu.make_async_copy(it_hbm, it_ref, row_sem.at[0]),
        pltpu.make_async_copy(tgt_hbm, tgt_ref, row_sem.at[1]),
    ]
    for q in range(parts):
        h_first(q, 0).start()
        w_copy(0, q).start()
    for q in range(parts):
        h_first(q, 1).start()
    for copy in row_copies:
        copy.start()
    def greet(k, carry_):
        pl.semaphore_signal(barrier, inc=1, device_id={"vp": (me + k) % size}, device_id_type=MESH)
        return carry_

    lax.fori_loop(1, size, greet, 0)
    r_iota = lax.broadcasted_iota(jnp.int32, (block, block), 0)
    c_iota = lax.broadcasted_iota(jnp.int32, (block, block), 1)
    tri_v[...] = jnp.where(r_iota <= c_iota, 1.0, 0.0).astype(BF16)

    lane = lax.broadcasted_iota(jnp.int32, (2 * rows, LANES), 1)

    def to_column(row):
        return jnp.transpose(jnp.broadcast_to(row, (LANES, LANES)))[:, :1]

    def row_params(p):
        chip = [chip_at(p, side) for side in range(2)]
        temp = [to_column(it_ref[pl.ds(k, 1)]) for k in chip]
        target = [to_column((tgt_ref[pl.ds(k, 1)] - me * local_vocab).astype(F32)) for k in chip]
        return jnp.concatenate(temp, axis=0), jnp.concatenate(target, axis=0)

    def product(p, j):
        start, width = bounds[j]
        return jnp.dot(hid_v[p], w_v[:, start : start + width], preferred_element_type=F32)

    def first_product(side):
        first_cols = pl.ds(0, bounds[0][1])
        mine = pl.ds(pl.multiple_of(side * rows, rows), rows)

        def add_piece(q, total):
            h_first(q, side).wait()

            @pl.when(side == 0)
            def _():
                w_copy(0, q).wait()
                w_copy(1, q).start()

            here = pl.ds(pl.multiple_of(q * piece, piece), piece)
            return total + jnp.dot(hid_v[0, mine, here], w_v[here, first_cols], preferred_element_type=F32)

        return lax.fori_loop(0, parts, add_piece, jnp.zeros((rows, bounds[0][1]), F32))

    def chunk(p, j, logits, temp, target, state, at=0):
        top, carry, pick = state
        count = logits.shape[0]
        first_col, width = bounds[j]
        logits = logits * temp
        new_top = jnp.maximum(top, jnp.max(logits, axis=1, keepdims=True))
        drop = jnp.exp(top - new_top)
        carry = carry * drop
        pick = pick * drop
        e = jnp.exp(logits - new_top)
        first = e.astype(BF16)
        rest = e - first.astype(F32)
        second = rest.astype(BF16)
        third = (rest - second.astype(F32)).astype(BF16)
        col = lax.broadcasted_iota(jnp.int32, (count, block), 1).astype(F32)
        for t in range(width // block):
            cut = slice(t * block, (t + 1) * block)
            terms = jnp.concatenate([first[:, cut], second[:, cut], third[:, cut]], axis=0)
            sums = jnp.dot(terms, tri_v[...], preferred_element_type=F32)
            run = (sums[:count] + (sums[count : 2 * count] + sums[2 * count :])) + carry
            base = first_col + t * block
            send_v[p, pl.ds(at, count), base : base + block] = run
            hit = (col + float(base)) == target
            pick = pick + jnp.sum(jnp.where(hit, run, 0.0), axis=1, keepdims=True)
            carry = run[:, block - 1 :]
        return new_top, carry, pick

    def send(p, side, columns, chip=None):
        chip = chip_at(p, side) if chip is None else chip
        for k in range(2):
            core = 1 - k
            pltpu.make_async_remote_copy(
                src_ref=send_v.at[p, pl.ds(pl.multiple_of(side * rows + core * half, half), half), columns],
                dst_ref=recv_ref.at[me, :, columns],
                send_sem=data_send.at[p, side],
                recv_sem=data_recv.at[me],
                device_id={"vp": chip * 2 + core},
                device_id_type=MESH,
            ).start()

    whole = pl.ds(0, local_vocab)

    def start_state(count):
        column = jnp.zeros((count, 1), F32)
        return column - jnp.inf, column, column

    def finish(p, tops, state):
        _, carry, pick = state
        stats = jnp.zeros((2 * rows, LANES), F32)
        for j in range(CHUNKS):
            stats = jnp.where(lane == j, tops[j], stats)
        stats = jnp.where(lane == CHUNKS, carry, stats)
        stats = jnp.where(lane == CHUNKS + 1, pick, stats)
        for side in range(2):
            stat_mine[c, p, side] = jnp.transpose(stats[side * rows : (side + 1) * rows])[:STATS]

    for copy in row_copies:
        copy.wait()

    def first_side(side, carry_):
        chip = chip_at(0, 0) * (1 - side) + chip_at(0, 1) * side
        temp = to_column(it_ref[pl.ds(chip, 1)])
        target = to_column((tgt_ref[pl.ds(chip, 1)] - me * local_vocab).astype(F32))
        at = pl.multiple_of(side * rows, rows)
        state = chunk(0, 0, first_product(side), temp, target, start_state(rows), at)
        for k, column in enumerate(state + (temp, target)):
            state_v[k, pl.ds(at, rows)] = column

        @pl.when(side == 0)
        def _():
            pl.semaphore_wait(barrier, size - 1)

        send(0, side, pl.ds(*bounds[0]), chip)
        return carry_

    lax.fori_loop(0, 2, first_side, 0)
    state = tuple(state_v[k] for k in range(3))
    temp0, target0 = state_v[3], state_v[4]
    tops = [state[0]]
    for j in range(2, CHUNKS):
        for q in range(parts):
            w_copy(j, q).start()
    for p in range(1, pairs):
        for side in range(2):
            h_copy(p, side).start()
    for j in range(1, CHUNKS):
        for q in range(parts):
            w_copy(j, q).wait()
        state = chunk(0, j, product(0, j), temp0, target0, state)
        tops.append(state[0])
        for side in range(2):
            send(0, side, pl.ds(*bounds[j]))
    finish(0, tops, state)

    def step(p, carry_):
        for side in range(2):
            h_copy(p, side).wait()
        temp, target = row_params(p)
        state = start_state(2 * rows)
        tops = []
        for j in range(CHUNKS):
            state = chunk(p, j, product(p, j), temp, target, state)
            tops.append(state[0])
        finish(p, tops, state)
        return carry_

    lax.fori_loop(1, pairs, step, 0)
    two, one, ends = range(1, pairs)
    others = [(p, side) for p in range(pairs) for side in range(2) if (p, side) != (ends, 0)]

    partner = z * 2 + (1 - c)

    def swap(k, mine, theirs):
        there = pltpu.make_async_remote_copy(
            src_ref=mine, dst_ref=mine, send_sem=pair_ssem.at[k], recv_sem=pair_rsem.at[k],
            device_id={"vp": partner}, device_id_type=MESH,
        )
        here = pltpu.make_async_remote_copy(
            src_ref=theirs, dst_ref=theirs, send_sem=pair_ssem.at[k], recv_sem=pair_rsem.at[k],
            device_id={"vp": partner}, device_id_type=MESH,
        )
        there.start()
        there.wait_send()
        here.wait_recv()

    swap(0, stat_mine.at[c], stat_mine.at[1 - c])

    def chip_on_side(p):
        steps = pairs - 1 - p
        return (z + (1 - 2 * c) * steps + c * pairs * (p // (pairs - 1)) + chips) % chips

    def stat_copy(p):
        return pltpu.make_async_remote_copy(
            src_ref=stat_mine.at[:, p, c],
            dst_ref=stat_recv.at[c, :, p],
            send_sem=stat_ssem.at[p],
            recv_sem=stat_rsem.at[p],
            device_id={"vp": chip_on_side(p) * 2 + c},
            device_id_type=MESH,
        )

    def t_copy(p):
        return pltpu.make_async_remote_copy(
            src_ref=t_mine,
            dst_ref=t_recv.at[c, pl.ds(p, 1)],
            send_sem=t_ssem.at[p],
            recv_sem=t_rsem.at[p],
            device_id={"vp": chip_on_side(p) * 2 + c},
            device_id_type=MESH,
        )

    def slot(chip):
        steps = (z - chip + chips) % chips
        side = steps // pairs
        return side, (1 - side) * (pairs - 1 - steps % pairs) + side * ((steps + pairs - 1) % pairs)

    for p in range(ends):
        stat_copy(p).start()

    @pl.when(c == 0)
    def _():
        stat_recv[0, :, ends] = stat_mine[:, ends, 0]

    @pl.when(c == 1)
    def _():
        stat_copy(ends).start()

    for side in range(2):
        send(one, side, whole)
    send(ends, 1, whole)

    theirs = pl.ds(pl.multiple_of((1 - c) * half, half), half)
    mine = pl.ds(pl.multiple_of(c * half, half), half)
    partner_data = pltpu.make_async_remote_copy(
        src_ref=send_v.at[ends, theirs],
        dst_ref=recv_ref.at[me],
        send_sem=data_send.at[ends, 0],
        recv_sem=data_recv.at[me],
        device_id={"vp": partner},
        device_id_type=MESH,
    )
    partner_data.start()
    recv_ref[me] = send_v[ends, mine]

    for p in range(ends):
        stat_copy(p).wait_recv()

    @pl.when(c == 1)
    def _():
        stat_copy(ends).wait_recv()

    swap(1, stat_recv.at[c], stat_recv.at[1 - c])
    shards = []
    for chip in range(chips):
        side, pair = slot(chip)
        shards += [stat_recv[side, core, pair] for core in range(2)]
    tops = [x[CHUNKS - 1 : CHUNKS] for x in shards]
    global_top = functools.reduce(jnp.maximum, tops)
    weights = [jnp.exp(t - global_top) for t in tops]
    masses = [x[CHUNKS : CHUNKS + 1] * w for x, w in zip(shards, weights)]
    inverse = 1.0 / functools.reduce(lambda a, b: a + b, masses)
    offsets = [jnp.zeros((1, rows), F32)]
    for s in range(size - 1):
        offsets.append(offsets[-1] + masses[s])
    ids = tgt_ref[pl.ds(z, 1)]
    value = jnp.zeros((1, rows), F32)
    for s in range(size):
        inside = (ids >= s * local_vocab) & (ids < (s + 1) * local_vocab)
        here = shards[s][CHUNKS + 1 : CHUNKS + 2] * weights[s] + offsets[s]
        value = value + jnp.where(inside, here, 0.0)
    t_mine[...] = value * inverse
    for p in range(ends):
        t_copy(p).start()

    @pl.when(c == 0)
    def _():
        t_recv[0, ends : ends + 1] = t_mine[...]

    @pl.when(c == 1)
    def _():
        t_copy(ends).start()

    for side in range(2):
        send(two, side, whole)

    scales = [jnp.exp(x[:CHUNKS] - global_top) * inverse for x in shards]
    table = jnp.concatenate(scales + [o * inverse for o in offsets], axis=0)
    pad = LANES - table.shape[0]
    if pad:
        table = jnp.concatenate([table, jnp.zeros((pad, rows), F32)], axis=0)
    turned = jnp.transpose(table)
    so_ref[...] = jnp.where(c == 0, turned[:half], turned[half:])

    for p in range(ends):
        t_copy(p).wait_recv()

    @pl.when(c == 1)
    def _():
        t_copy(ends).wait_recv()

    swap(2, t_recv.at[c], t_recv.at[1 - c])
    for chip in range(chips):
        side, pair = slot(chip)
        out_t_ref[chip : chip + 1] = t_recv[side, pl.ds(pair, 1)]
    for p in range(ends):
        stat_copy(p).wait_send()
        t_copy(p).wait_send()

    @pl.when(c == 1)
    def _():
        stat_copy(ends).wait_send()
        t_copy(ends).wait_send()

    for p, side in others:
        gone = send_v.at[p, pl.ds(side * rows, rows)]
        pltpu.make_async_remote_copy(
            src_ref=gone, dst_ref=gone, send_sem=data_send.at[p, side], recv_sem=data_recv.at[0],
            device_id={"vp": chip_at(p, side) * 2}, device_id_type=MESH,
        ).wait_send()
    partner_data.wait_send()

    def wait_data(k, carry_):
        src = (me + k) % size
        there = recv_ref.at[src]
        pltpu.make_async_remote_copy(
            src_ref=there, dst_ref=there, send_sem=data_send.at[0, 0], recv_sem=data_recv.at[src],
            device_id={"vp": src}, device_id_type=MESH,
        ).wait_recv()
        return carry_

    lax.fori_loop(1, size, wait_data, 0)


def table_kernel(size, recv_ref, so_ref, t_ref, table_ref, out_t_ref, stage, sems, t_sem):
    shard = recv_ref.shape[2]
    t_out = pltpu.make_async_copy(t_ref, out_t_ref, t_sem)
    t_out.start()
    copies = []
    for s in range(size):
        offset = so_ref[:, size * CHUNKS + s : size * CHUNKS + s + 1]
        for j, (start, width) in enumerate(chunk_bounds(shard)):
            k = s * CHUNKS + j
            cut = slice(start, start + width)
            stage[s, :, cut] = recv_ref[s, :, cut] * so_ref[:, k : k + 1] + offset
        copy = pltpu.make_async_copy(stage.at[s], table_ref.at[:, pl.ds(s * shard, shard)], sems.at[s])
        copy.start()
        copies.append(copy)
    t_out.wait()
    for copy in copies:
        copy.wait()


def solution(mesh):
    size = mesh.shape["vp"]
    chips = size // 2
    assert chips == 8

    def local_step(hidden, w_local, inv_temp, target_ids):
        batch, depth = hidden.shape
        local_vocab = w_local.shape[1]
        rows = batch // chips
        half = rows // 2
        block = min(256, local_vocab // 8)
        vmem = pl.BlockSpec(memory_space=pltpu.VMEM)
        hbm = pl.BlockSpec(memory_space=pl.ANY)
        recv, so, t_all = pl.pallas_call(
            functools.partial(exchange_kernel, size),
            out_shape=(
                pltpu.VMEM((size, half, local_vocab), F32),
                pltpu.VMEM((half, LANES), F32),
                pltpu.VMEM((chips, rows), F32),
            ),
            in_specs=[hbm, hbm, hbm, hbm],
            out_specs=(vmem, vmem, vmem),
            scratch_shapes=[
                pltpu.VMEM((chips, rows), F32),
                pltpu.VMEM((chips, rows), jnp.int32),
                pltpu.VMEM((depth, local_vocab), BF16),
                pltpu.VMEM((chips // 2, 2 * rows, depth), BF16),
                pltpu.VMEM((block, block), BF16),
                pltpu.VMEM((5, 2 * rows, 1), F32),
                pltpu.VMEM((chips // 2, 2 * rows, local_vocab), F32),
                pltpu.VMEM((2, chips // 2, 2, STATS, rows), F32),
                pltpu.VMEM((2, 2, chips // 2, STATS, rows), F32),
                pltpu.VMEM((1, rows), F32),
                pltpu.VMEM((2, chips // 2, rows), F32),
                pltpu.SemaphoreType.DMA((2,)),
                pltpu.SemaphoreType.DMA((CHUNKS, 4)),
                pltpu.SemaphoreType.DMA((chips // 2, 2)),
                pltpu.SemaphoreType.DMA((4, 2)),
                pltpu.SemaphoreType.DMA((chips // 2, 2)),
                pltpu.SemaphoreType.DMA((size,)),
                pltpu.SemaphoreType.DMA((chips // 2,)),
                pltpu.SemaphoreType.DMA((chips // 2,)),
                pltpu.SemaphoreType.DMA((3,)),
                pltpu.SemaphoreType.DMA((3,)),
                pltpu.SemaphoreType.DMA((chips // 2,)),
                pltpu.SemaphoreType.DMA((chips // 2,)),
            ],
            compiler_params=pltpu.CompilerParams(
                collective_id=0, has_side_effects=True, vmem_limit_bytes=46 * 1024 * 1024
            ),
            name="exchange",
        )(inv_temp.reshape(chips, rows), target_ids.reshape(chips, rows), hidden, w_local)
        recv, so, t_all = [pltpu.with_memory_space_constraint(x, pltpu.VMEM) for x in (recv, so, t_all)]
        table, cdf_at_target = pl.pallas_call(
            functools.partial(table_kernel, size),
            out_shape=(
                jax.ShapeDtypeStruct((half, size * local_vocab), F32),
                jax.ShapeDtypeStruct((chips, rows), F32),
            ),
            in_specs=[vmem, vmem, vmem],
            out_specs=(hbm, hbm),
            scratch_shapes=[
                pltpu.VMEM((size, half, local_vocab), F32),
                pltpu.SemaphoreType.DMA((size,)),
                pltpu.SemaphoreType.DMA,
            ],
            compiler_params=pltpu.CompilerParams(vmem_limit_bytes=24 * 1024 * 1024),
            name="table",
        )(recv, so, t_all)
        return table, cdf_at_target.reshape(batch)

    return jax.shard_map(
        local_step,
        mesh=mesh,
        in_specs=(P("dp", None), P(None, "vp"), P("dp"), P("dp")),
        out_specs=(P(("dp", "vp"), None), P("dp")),
        check_vma=False,
    )
```

```python
import functools
import jax
import jax.numpy as jnp
from jax import lax
from jax.experimental import pallas as pl
from jax.experimental.pallas import tpu as pltpu
from jax.sharding import PartitionSpec as P

MESH = pl.DeviceIdType.MESH
F32 = jnp.float32
BF16 = jnp.bfloat16
LANES = 128
SIXTEENTHS = (1, 5, 10)
CHUNKS = len(SIXTEENTHS)
STATS = CHUNKS + 2


def chunk_bounds(local_vocab):
    bounds, start = [], 0
    for part in SIXTEENTHS:
        bounds.append((start, part * local_vocab // 16))
        start += part * local_vocab // 16
    return bounds


def exchange_kernel(
    size, it_hbm, tgt_hbm, hid_ref, w_ref,
    recv_ref, so_ref, out_t_ref,
    it_ref, tgt_ref, w_v, hid_v, tri_v, state_v, send_v, stat_mine, stat_recv, t_mine, t_recv,
    row_sem, w_sem, h_sem, h0_sem, data_send, data_recv, here_sem, stat_ssem, stat_rsem, pair_ssem, pair_rsem, t_ssem, t_rsem,
):
    me = lax.axis_index("vp")
    chips = size // 2
    z, c = me // 2, me % 2
    rows = hid_ref.shape[0] // chips
    half = rows // 2
    depth = hid_ref.shape[1]
    local_vocab = w_ref.shape[1]
    bounds = chunk_bounds(local_vocab)
    block = tri_v.shape[0]

    pairs = chips // 2

    def chip_at(p, side):
        steps = pairs - 1 - p
        return (z + steps) % chips if side == 0 else (z - steps + pairs * (p // (pairs - 1)) + chips) % chips

    barrier = pltpu.get_barrier_semaphore()
    parts = w_sem.shape[1]
    piece = depth // parts

    def w_copy(j, p):
        start, width = bounds[j]
        here = (pl.ds(pl.multiple_of(p * piece, piece), piece), pl.ds(start, width))
        return pltpu.make_async_copy(w_ref.at[here], w_v.at[here], w_sem.at[j, p])

    def h_copy(p, side):
        start = pl.multiple_of(chip_at(p, side) * rows, rows)
        return pltpu.make_async_copy(
            hid_ref.at[pl.ds(start, rows)], hid_v.at[p, pl.ds(side * rows, rows)], h_sem.at[p, side]
        )

    def h_first(q, side):
        chip = chip_at(0, 0) * (1 - side) + chip_at(0, 1) * side
        start = pl.multiple_of(chip * rows, rows)
        here = pl.ds(pl.multiple_of(q * piece, piece), piece)
        there = pl.ds(pl.multiple_of(side * rows, rows), rows)
        return pltpu.make_async_copy(
            hid_ref.at[pl.ds(start, rows), here], hid_v.at[0, there, here], h0_sem.at[q, side]
        )

    row_copies = [
        pltpu.make_async_copy(it_hbm, it_ref, row_sem.at[0]),
        pltpu.make_async_copy(tgt_hbm, tgt_ref, row_sem.at[1]),
    ]
    for q in range(parts):
        h_first(q, 0).start()
        w_copy(0, q).start()
    for q in range(parts):
        h_first(q, 1).start()
    for copy in row_copies:
        copy.start()
    def ahead(steps, core):
        return ((z + steps + chips) % chips) * 2 + core

    for peer in [ahead(d, core) for d in (pairs - 1, 1 - pairs) for core in range(2)] + [z * 2 + (1 - c)]:
        pl.semaphore_signal(barrier, inc=1, device_id={"vp": peer}, device_id_type=MESH)
    r_iota = lax.broadcasted_iota(jnp.int32, (block, block), 0)
    c_iota = lax.broadcasted_iota(jnp.int32, (block, block), 1)
    tri_v[...] = jnp.where(r_iota <= c_iota, 1.0, 0.0).astype(BF16)

    lane = lax.broadcasted_iota(jnp.int32, (2 * rows, LANES), 1)

    def to_column(row):
        return jnp.transpose(jnp.broadcast_to(row, (LANES, LANES)))[:, :1]

    def row_params(p):
        chip = [chip_at(p, side) for side in range(2)]
        temp = [to_column(it_ref[pl.ds(k, 1)]) for k in chip]
        target = [to_column((tgt_ref[pl.ds(k, 1)] - me * local_vocab).astype(F32)) for k in chip]
        return jnp.concatenate(temp, axis=0), jnp.concatenate(target, axis=0)

    def product(p, j):
        start, width = bounds[j]
        return jnp.dot(hid_v[p], w_v[:, start : start + width], preferred_element_type=F32)

    def first_product(side):
        first_cols = pl.ds(0, bounds[0][1])
        mine = pl.ds(pl.multiple_of(side * rows, rows), rows)

        def add_piece(q, total):
            h_first(q, side).wait()

            @pl.when(side == 0)
            def _():
                w_copy(0, q).wait()
                w_copy(1, q).start()

            here = pl.ds(pl.multiple_of(q * piece, piece), piece)
            return total + jnp.dot(hid_v[0, mine, here], w_v[here, first_cols], preferred_element_type=F32)

        return lax.fori_loop(0, parts, add_piece, jnp.zeros((rows, bounds[0][1]), F32))

    def chunk(p, j, logits, temp, target, state, at=0):
        top, carry, pick = state
        count = logits.shape[0]
        first_col, width = bounds[j]
        logits = logits * temp
        new_top = jnp.maximum(top, jnp.max(logits, axis=1, keepdims=True))
        drop = jnp.exp(top - new_top)
        carry = carry * drop
        pick = pick * drop
        e = jnp.exp(logits - new_top)
        first = e.astype(BF16)
        rest = e - first.astype(F32)
        second = rest.astype(BF16)
        third = (rest - second.astype(F32)).astype(BF16)
        col = lax.broadcasted_iota(jnp.int32, (count, block), 1).astype(F32)
        for t in range(width // block):
            cut = slice(t * block, (t + 1) * block)
            terms = jnp.concatenate([first[:, cut], second[:, cut], third[:, cut]], axis=0)
            sums = jnp.dot(terms, tri_v[...], preferred_element_type=F32)
            run = (sums[:count] + (sums[count : 2 * count] + sums[2 * count :])) + carry
            base = first_col + t * block
            send_v[p, pl.ds(at, count), base : base + block] = run
            hit = (col + float(base)) == target
            pick = pick + jnp.sum(jnp.where(hit, run, 0.0), axis=1, keepdims=True)
            carry = run[:, block - 1 :]
        return new_top, carry, pick

    def send(p, side, columns, chip=None):
        chip = chip_at(p, side) if chip is None else chip
        for k in range(2):
            core = 1 - k
            pltpu.make_async_remote_copy(
                src_ref=send_v.at[p, pl.ds(pl.multiple_of(side * rows + core * half, half), half), columns],
                dst_ref=recv_ref.at[me, :, columns],
                send_sem=data_send.at[p, side],
                recv_sem=data_recv.at[me],
                device_id={"vp": chip * 2 + core},
                device_id_type=MESH,
            ).start()

    whole = pl.ds(0, local_vocab)

    def start_state(count):
        column = jnp.zeros((count, 1), F32)
        return column - jnp.inf, column, column

    def finish(p, tops, state):
        _, carry, pick = state
        stats = jnp.zeros((2 * rows, LANES), F32)
        for j in range(CHUNKS):
            stats = jnp.where(lane == j, tops[j], stats)
        stats = jnp.where(lane == CHUNKS, carry, stats)
        stats = jnp.where(lane == CHUNKS + 1, pick, stats)
        for side in range(2):
            stat_mine[c, p, side] = jnp.transpose(stats[side * rows : (side + 1) * rows])[:STATS]

    for copy in row_copies:
        copy.wait()

    def first_side(side, carry_):
        chip = chip_at(0, 0) * (1 - side) + chip_at(0, 1) * side
        temp = to_column(it_ref[pl.ds(chip, 1)])
        target = to_column((tgt_ref[pl.ds(chip, 1)] - me * local_vocab).astype(F32))
        at = pl.multiple_of(side * rows, rows)
        state = chunk(0, 0, first_product(side), temp, target, start_state(rows), at)
        for k, column in enumerate(state + (temp, target)):
            state_v[k, pl.ds(at, rows)] = column

        @pl.when(side == 0)
        def _():
            pl.semaphore_wait(barrier, 5)

        send(0, side, pl.ds(*bounds[0]), chip)
        return carry_

    lax.fori_loop(0, 2, first_side, 0)
    for d in (pairs - 1, 1 - pairs):
        pl.semaphore_signal(here_sem.at[0], inc=1, device_id={"vp": ahead(d, c)}, device_id_type=MESH)
    state = tuple(state_v[k] for k in range(3))
    temp0, target0 = state_v[3], state_v[4]
    tops = [state[0]]
    for j in range(2, CHUNKS):
        for q in range(parts):
            w_copy(j, q).start()
    for p in range(1, pairs):
        for side in range(2):
            h_copy(p, side).start()
    for j in range(1, CHUNKS):
        for q in range(parts):
            w_copy(j, q).wait()
        state = chunk(0, j, product(0, j), temp0, target0, state)
        tops.append(state[0])
        for side in range(2):
            send(0, side, pl.ds(*bounds[j]))
    finish(0, tops, state)
    pl.semaphore_wait(here_sem.at[0], 2)
    for d in (2, -2):
        pl.semaphore_signal(here_sem.at[1], inc=1, device_id={"vp": ahead(d, c)}, device_id_type=MESH)

    def step(p, carry_):
        for side in range(2):
            h_copy(p, side).wait()
        temp, target = row_params(p)
        state = start_state(2 * rows)
        tops = []
        for j in range(CHUNKS):
            state = chunk(p, j, product(p, j), temp, target, state)
            tops.append(state[0])
        finish(p, tops, state)
        return carry_

    lax.fori_loop(1, pairs, step, 0)
    pl.semaphore_wait(here_sem.at[1], 2)
    two, one, ends = range(1, pairs)
    others = [(p, side) for p in range(pairs) for side in range(2) if (p, side) != (ends, 0)]

    partner = z * 2 + (1 - c)

    def swap(k, mine, theirs):
        there = pltpu.make_async_remote_copy(
            src_ref=mine, dst_ref=mine, send_sem=pair_ssem.at[k], recv_sem=pair_rsem.at[k],
            device_id={"vp": partner}, device_id_type=MESH,
        )
        here = pltpu.make_async_remote_copy(
            src_ref=theirs, dst_ref=theirs, send_sem=pair_ssem.at[k], recv_sem=pair_rsem.at[k],
            device_id={"vp": partner}, device_id_type=MESH,
        )
        there.start()
        there.wait_send()
        here.wait_recv()

    swap(0, stat_mine.at[c], stat_mine.at[1 - c])

    def chip_on_side(p):
        steps = pairs - 1 - p
        return (z + (1 - 2 * c) * steps + c * pairs * (p // (pairs - 1)) + chips) % chips

    def stat_copy(p):
        return pltpu.make_async_remote_copy(
            src_ref=stat_mine.at[:, p, c],
            dst_ref=stat_recv.at[c, :, p],
            send_sem=stat_ssem.at[p],
            recv_sem=stat_rsem.at[p],
            device_id={"vp": chip_on_side(p) * 2 + c},
            device_id_type=MESH,
        )

    def t_copy(p):
        return pltpu.make_async_remote_copy(
            src_ref=t_mine,
            dst_ref=t_recv.at[c, pl.ds(p, 1)],
            send_sem=t_ssem.at[p],
            recv_sem=t_rsem.at[p],
            device_id={"vp": chip_on_side(p) * 2 + c},
            device_id_type=MESH,
        )

    def slot(chip):
        steps = (z - chip + chips) % chips
        side = steps // pairs
        return side, (1 - side) * (pairs - 1 - steps % pairs) + side * ((steps + pairs - 1) % pairs)

    for p in range(ends):
        stat_copy(p).start()

    @pl.when(c == 0)
    def _():
        stat_recv[0, :, ends] = stat_mine[:, ends, 0]

    @pl.when(c == 1)
    def _():
        stat_copy(ends).start()

    for side in range(2):
        send(one, side, whole)
    send(ends, 1, whole)

    theirs = pl.ds(pl.multiple_of((1 - c) * half, half), half)
    mine = pl.ds(pl.multiple_of(c * half, half), half)
    partner_data = pltpu.make_async_remote_copy(
        src_ref=send_v.at[ends, theirs],
        dst_ref=recv_ref.at[me],
        send_sem=data_send.at[ends, 0],
        recv_sem=data_recv.at[me],
        device_id={"vp": partner},
        device_id_type=MESH,
    )
    partner_data.start()
    recv_ref[me] = send_v[ends, mine]

    for p in range(ends):
        stat_copy(p).wait_recv()

    @pl.when(c == 1)
    def _():
        stat_copy(ends).wait_recv()

    swap(1, stat_recv.at[c], stat_recv.at[1 - c])
    shards = []
    for chip in range(chips):
        side, pair = slot(chip)
        shards += [stat_recv[side, core, pair] for core in range(2)]
    tops = [x[CHUNKS - 1 : CHUNKS] for x in shards]
    global_top = functools.reduce(jnp.maximum, tops)
    weights = [jnp.exp(t - global_top) for t in tops]
    masses = [x[CHUNKS : CHUNKS + 1] * w for x, w in zip(shards, weights)]
    inverse = 1.0 / functools.reduce(lambda a, b: a + b, masses)
    offsets = [jnp.zeros((1, rows), F32)]
    for s in range(size - 1):
        offsets.append(offsets[-1] + masses[s])
    ids = tgt_ref[pl.ds(z, 1)]
    value = jnp.zeros((1, rows), F32)
    for s in range(size):
        inside = (ids >= s * local_vocab) & (ids < (s + 1) * local_vocab)
        here = shards[s][CHUNKS + 1 : CHUNKS + 2] * weights[s] + offsets[s]
        value = value + jnp.where(inside, here, 0.0)
    t_mine[...] = value * inverse
    for p in range(ends):
        t_copy(p).start()

    @pl.when(c == 0)
    def _():
        t_recv[0, ends : ends + 1] = t_mine[...]

    @pl.when(c == 1)
    def _():
        t_copy(ends).start()

    for side in range(2):
        send(two, side, whole)

    scales = [jnp.exp(x[:CHUNKS] - global_top) * inverse for x in shards]
    table = jnp.concatenate(scales + [o * inverse for o in offsets], axis=0)
    pad = LANES - table.shape[0]
    if pad:
        table = jnp.concatenate([table, jnp.zeros((pad, rows), F32)], axis=0)
    turned = jnp.transpose(table)
    so_ref[...] = jnp.where(c == 0, turned[:half], turned[half:])

    for p in range(ends):
        t_copy(p).wait_recv()

    @pl.when(c == 1)
    def _():
        t_copy(ends).wait_recv()

    swap(2, t_recv.at[c], t_recv.at[1 - c])
    for chip in range(chips):
        side, pair = slot(chip)
        out_t_ref[chip : chip + 1] = t_recv[side, pl.ds(pair, 1)]
    for p in range(ends):
        stat_copy(p).wait_send()
        t_copy(p).wait_send()

    @pl.when(c == 1)
    def _():
        stat_copy(ends).wait_send()
        t_copy(ends).wait_send()

    for p, side in others:
        gone = send_v.at[p, pl.ds(side * rows, rows)]
        pltpu.make_async_remote_copy(
            src_ref=gone, dst_ref=gone, send_sem=data_send.at[p, side], recv_sem=data_recv.at[0],
            device_id={"vp": chip_at(p, side) * 2}, device_id_type=MESH,
        ).wait_send()
    partner_data.wait_send()

    def wait_data(k, carry_):
        src = (me + k) % size
        there = recv_ref.at[src]
        pltpu.make_async_remote_copy(
            src_ref=there, dst_ref=there, send_sem=data_send.at[0, 0], recv_sem=data_recv.at[src],
            device_id={"vp": src}, device_id_type=MESH,
        ).wait_recv()
        return carry_

    lax.fori_loop(1, size, wait_data, 0)


def table_kernel(size, recv_ref, so_ref, t_ref, table_ref, out_t_ref, stage, sems, t_sem):
    shard = recv_ref.shape[2]
    t_out = pltpu.make_async_copy(t_ref, out_t_ref, t_sem)
    t_out.start()
    copies = []
    for s in range(size):
        offset = so_ref[:, size * CHUNKS + s : size * CHUNKS + s + 1]
        for j, (start, width) in enumerate(chunk_bounds(shard)):
            k = s * CHUNKS + j
            cut = slice(start, start + width)
            stage[s, :, cut] = recv_ref[s, :, cut] * so_ref[:, k : k + 1] + offset
        copy = pltpu.make_async_copy(stage.at[s], table_ref.at[:, pl.ds(s * shard, shard)], sems.at[s])
        copy.start()
        copies.append(copy)
    t_out.wait()
    for copy in copies:
        copy.wait()


def solution(mesh):
    size = mesh.shape["vp"]
    chips = size // 2
    assert chips == 8

    def local_step(hidden, w_local, inv_temp, target_ids):
        batch, depth = hidden.shape
        local_vocab = w_local.shape[1]
        rows = batch // chips
        half = rows // 2
        block = min(256, local_vocab // 16)
        vmem = pl.BlockSpec(memory_space=pltpu.VMEM)
        hbm = pl.BlockSpec(memory_space=pl.ANY)
        recv, so, t_all = pl.pallas_call(
            functools.partial(exchange_kernel, size),
            out_shape=(
                pltpu.VMEM((size, half, local_vocab), F32),
                pltpu.VMEM((half, LANES), F32),
                pltpu.VMEM((chips, rows), F32),
            ),
            in_specs=[hbm, hbm, hbm, hbm],
            out_specs=(vmem, vmem, vmem),
            scratch_shapes=[
                pltpu.VMEM((chips, rows), F32),
                pltpu.VMEM((chips, rows), jnp.int32),
                pltpu.VMEM((depth, local_vocab), BF16),
                pltpu.VMEM((chips // 2, 2 * rows, depth), BF16),
                pltpu.VMEM((block, block), BF16),
                pltpu.VMEM((5, 2 * rows, 1), F32),
                pltpu.VMEM((chips // 2, 2 * rows, local_vocab), F32),
                pltpu.VMEM((2, chips // 2, 2, STATS, rows), F32),
                pltpu.VMEM((2, 2, chips // 2, STATS, rows), F32),
                pltpu.VMEM((1, rows), F32),
                pltpu.VMEM((2, chips // 2, rows), F32),
                pltpu.SemaphoreType.DMA((2,)),
                pltpu.SemaphoreType.DMA((CHUNKS, 4)),
                pltpu.SemaphoreType.DMA((chips // 2, 2)),
                pltpu.SemaphoreType.DMA((4, 2)),
                pltpu.SemaphoreType.DMA((chips // 2, 2)),
                pltpu.SemaphoreType.DMA((size,)),
                pltpu.SemaphoreType.REGULAR((2,)),
                pltpu.SemaphoreType.DMA((chips // 2,)),
                pltpu.SemaphoreType.DMA((chips // 2,)),
                pltpu.SemaphoreType.DMA((3,)),
                pltpu.SemaphoreType.DMA((3,)),
                pltpu.SemaphoreType.DMA((chips // 2,)),
                pltpu.SemaphoreType.DMA((chips // 2,)),
            ],
            compiler_params=pltpu.CompilerParams(
                collective_id=0, has_side_effects=True, vmem_limit_bytes=46 * 1024 * 1024
            ),
            name="exchange",
        )(inv_temp.reshape(chips, rows), target_ids.reshape(chips, rows), hidden, w_local)
        recv, so, t_all = [pltpu.with_memory_space_constraint(x, pltpu.VMEM) for x in (recv, so, t_all)]
        table, cdf_at_target = pl.pallas_call(
            functools.partial(table_kernel, size),
            out_shape=(
                jax.ShapeDtypeStruct((half, size * local_vocab), F32),
                jax.ShapeDtypeStruct((chips, rows), F32),
            ),
            in_specs=[vmem, vmem, vmem],
            out_specs=(hbm, hbm),
            scratch_shapes=[
                pltpu.VMEM((size, half, local_vocab), F32),
                pltpu.SemaphoreType.DMA((size,)),
                pltpu.SemaphoreType.DMA,
            ],
            compiler_params=pltpu.CompilerParams(vmem_limit_bytes=24 * 1024 * 1024),
            name="table",
        )(recv, so, t_all)
        return table, cdf_at_target.reshape(batch)

    return jax.shard_map(
        local_step,
        mesh=mesh,
        in_specs=(P("dp", None), P(None, "vp"), P("dp"), P("dp")),
        out_specs=(P(("dp", "vp"), None), P("dp")),
        check_vma=False,
    )
```
